32 devices in a mesh: tok: 8 (over z, y), head: 4 (over x, core).
Axes of the slice: x: 2, y: 2, z: 4, core: 2. Of those that a mesh axis runs over, the one named last changes fastest.
Arguments:
- query_rows: bfloat16 [4096, 4, 1024], P('tok', 'head'), may hold values from -6 to 6
- key_rows: bfloat16 [4096, 4, 128], P('tok', 'head'), may hold values from -6 to 6
- value_rows: bfloat16 [4096, 4, 128], P('tok', 'head'), may hold values from -6 to 6
- output_gradient: bfloat16 [4096, 4, 1024], P('tok', 'head'), may hold values from -6 to 6
- row_logsumexp: bfloat16 [4, 8, 4096], P('head', None, 'tok'), may hold values from 3 to 7
- row_delta_sums: bfloat16 [4, 8, 4096], P('head', None, 'tok'), may hold values from -5 to 5
- segments: int32 [4096], replicated, may hold values from 0 to 4095, as said below
- query_key_value_weight: bfloat16 [4096, 4, 1280], P('tok', 'head'), may hold values from -0.09375 to 0.09375
Outputs:
- grad_input: bfloat16 [4096, 4096], P('tok', 'head')
The draws below stay inside these ranges and needn't reach their ends.
Inputs may be any that keep to these rules, and one draw needn't show every extreme that they name: `segments`: numbers never fall along the tokens, and every document lies inside one window of 512 consecutive tokens.
All inputs are finite; a program needn't handle non-finite values.
Results may differ from the reference program's by a relative error of at most 0.012.
Values may be sent and summed in bfloat16 or wider, within the bound.
A program may use at most 128 MiB of HBM per device.

```python
import jax
import jax.numpy as jnp
from jax import lax

MODEL_WIDTH = 4096
QUERY_HEADS = 32
KEY_VALUE_HEADS = 4
HEAD_WIDTH = 128
BLOCK = 128
WINDOW_TOKENS = 512
GROUP_KV_HEADS = 1
TOKEN_TOTAL = 4096
N_TOK = 8


def document_plan(key):
    windows = TOKEN_TOTAL // WINDOW_TOKENS
    half_axis = windows // 2
    window_ids = jnp.arange(windows, dtype=jnp.int32)
    positions = jnp.arange(WINDOW_TOKENS, dtype=jnp.int32)
    sparse_density = jax.random.randint(jax.random.fold_in(key, 11), (windows, 1), 0, 2)
    dense_density = jax.random.randint(jax.random.fold_in(key, 13), (windows, 1), 64, 193)
    density = jnp.where(window_ids[:, None] < half_axis, sparse_density, dense_density)
    rolls = jax.random.randint(jax.random.fold_in(key, 12), (windows, WINDOW_TOKENS), 0, 64 * BLOCK)
    cut_flags = (rolls < density) & (positions[None, :] > 0)
    block_cuts = (positions % BLOCK == 0) & (positions > 0)
    cut_flags = jnp.where(window_ids[:, None] == 0, False, cut_flags)
    cut_flags = jnp.where(window_ids[:, None] == half_axis, block_cuts[None, :], cut_flags)
    local_ids = jnp.cumsum(cut_flags.astype(jnp.int32), axis=1)
    return local_ids + window_ids[:, None] * WINDOW_TOKENS


def draw_segments(key, part):
    return document_plan(key).reshape(TOKEN_TOTAL).astype(jnp.int32)


def levels(stream_key, dims, split, smallest, top_value):
    factor_of, own = 1.0, jax.random.fold_in(stream_key, 6)
    for position, shards_of in split:
        heights = jnp.exp(jax.random.uniform(jax.random.fold_in(own, position), (shards_of,), jnp.float32, smallest / len(split), top_value / len(split)))
        factor_of = factor_of * jnp.repeat(heights, dims[position] // shards_of).reshape([-1 if axis == position else 1 for axis in range(len(dims))])
    return factor_of


def scatter_about(rng, dims, deviation, most, shards=(), held_as=jnp.bfloat16):
    loudness = levels(rng, dims, shards, -0.22, 0.18) if shards else 1.0
    array = jax.random.normal(rng, dims, jnp.float32) * deviation * loudness
    return jnp.minimum(jnp.maximum(array, -most), most).astype(held_as)


def setup_inputs(seed: int = 0) -> dict:
    keys = jax.random.split(jax.random.key(seed), 9)
    return {
        "query_rows": scatter_about(keys[0], (TOKEN_TOTAL, KEY_VALUE_HEADS, QUERY_HEADS // KEY_VALUE_HEADS * HEAD_WIDTH), 1.0, 6.0, ((0, 8), (1, 4))),
        "key_rows": scatter_about(keys[1], (TOKEN_TOTAL, KEY_VALUE_HEADS, HEAD_WIDTH), 1.0, 6.0, ((0, 8), (1, 4))),
        "value_rows": scatter_about(keys[2], (TOKEN_TOTAL, KEY_VALUE_HEADS, HEAD_WIDTH), 1.0, 6.0, ((0, 8), (1, 4))),
        "output_gradient": scatter_about(keys[3], (TOKEN_TOTAL, KEY_VALUE_HEADS, QUERY_HEADS // KEY_VALUE_HEADS * HEAD_WIDTH), 1.0, 6.0, ((0, 8), (1, 4))),
        "row_logsumexp": jnp.clip(3.0 + 4.0 * jax.random.uniform(keys[4], (KEY_VALUE_HEADS, QUERY_HEADS // KEY_VALUE_HEADS, TOKEN_TOTAL), jnp.float32) ** levels(keys[4], (KEY_VALUE_HEADS, QUERY_HEADS // KEY_VALUE_HEADS, TOKEN_TOTAL), ((0, 4), (2, 8)), -0.2, 0.2), 3.0, 7.0).astype(jnp.bfloat16),
        "row_delta_sums": scatter_about(keys[5], (KEY_VALUE_HEADS, QUERY_HEADS // KEY_VALUE_HEADS, TOKEN_TOTAL), 1.0, 5.0, ((0, 4), (2, 8))),
        "segments": draw_segments(jax.random.fold_in(keys[8], 71), 0),
        "query_key_value_weight": scatter_about(keys[7], (MODEL_WIDTH, KEY_VALUE_HEADS, (QUERY_HEADS // KEY_VALUE_HEADS + 2) * HEAD_WIDTH), MODEL_WIDTH ** -0.5, 0.09375, ((0, 8), (1, 4))),
    }


def reference(query_rows, key_rows, value_rows, output_gradient, row_logsumexp, row_delta_sums, segments, query_key_value_weight):
    heads_per_group = QUERY_HEADS // KEY_VALUE_HEADS
    score_scale = HEAD_WIDTH ** -0.5
    offsets = jnp.arange(WINDOW_TOKENS)
    causal = offsets[None, :] <= offsets[:, None]

    def one_window(window_index):
        leading_row = (window_index * WINDOW_TOKENS).astype(jnp.int32)
        query_window_rows = lax.dynamic_slice_in_dim(query_rows, leading_row, WINDOW_TOKENS, 0).astype(jnp.float32).reshape(WINDOW_TOKENS, KEY_VALUE_HEADS, heads_per_group, HEAD_WIDTH)
        output_grad_window = lax.dynamic_slice_in_dim(output_gradient, leading_row, WINDOW_TOKENS, 0).astype(jnp.float32).reshape(WINDOW_TOKENS, KEY_VALUE_HEADS, heads_per_group, HEAD_WIDTH)
        key_win = lax.dynamic_slice_in_dim(key_rows, leading_row, WINDOW_TOKENS, 0).astype(jnp.float32)
        value_win = lax.dynamic_slice_in_dim(value_rows, leading_row, WINDOW_TOKENS, 0).astype(jnp.float32)
        lse_win = lax.dynamic_slice_in_dim(row_logsumexp, leading_row, WINDOW_TOKENS, 2).astype(jnp.float32)
        delta_win = lax.dynamic_slice_in_dim(row_delta_sums, leading_row, WINDOW_TOKENS, 2).astype(jnp.float32)
        seg_win = lax.dynamic_slice_in_dim(segments, leading_row, WINDOW_TOKENS, 0)
        allowed = (seg_win[:, None] == seg_win[None, :]) & causal
        scores = jnp.einsum("agrd,bgd->grab", query_window_rows, key_win) * score_scale
        soft_probs = jnp.where(allowed[None, None], jnp.exp(scores - lse_win[..., None]), 0.0)
        probs_low = lax.optimization_barrier(soft_probs.astype(jnp.bfloat16)).astype(jnp.float32)
        value_gradient = jnp.einsum("grab,agrd->bgd", probs_low, output_grad_window)
        grad_prob = jnp.einsum("agrd,bgd->grab", output_grad_window, value_win)
        grad_score = soft_probs * (grad_prob - delta_win[..., None])
        score_low = lax.optimization_barrier(grad_score.astype(jnp.bfloat16)).astype(jnp.float32)
        query_gradient = jnp.einsum("grab,bgd->agrd", score_low, key_win) * score_scale
        key_gradient = jnp.einsum("grab,agrd->bgd", score_low, query_window_rows) * score_scale
        stacked_gradients = jnp.concatenate([query_gradient.reshape(WINDOW_TOKENS, KEY_VALUE_HEADS, heads_per_group * HEAD_WIDTH), key_gradient, value_gradient], axis=2).astype(jnp.bfloat16)
        running_sum = jnp.zeros((WINDOW_TOKENS, MODEL_WIDTH), jnp.float32)
        for group_of_heads in range(KEY_VALUE_HEADS // GROUP_KV_HEADS):
            first_head = group_of_heads * GROUP_KV_HEADS
            part_rows = stacked_gradients[:, first_head:first_head + GROUP_KV_HEADS, :].reshape(WINDOW_TOKENS, -1)
            part_weights = query_key_value_weight[:, first_head:first_head + GROUP_KV_HEADS, :].reshape(MODEL_WIDTH, -1)
            group_term = jnp.dot(part_rows, part_weights.T, preferred_element_type=jnp.float32)
            running_sum = running_sum + lax.optimization_barrier(group_term.astype(jnp.bfloat16)).astype(jnp.float32)
        return running_sum.astype(jnp.bfloat16)

    return lax.map(one_window, jnp.arange(N_TOK, dtype=jnp.int32)).reshape(TOKEN_TOTAL, MODEL_WIDTH)
```

```python
import functools

import jax
import jax.numpy as jnp
import numpy as np
from jax import lax
from jax.experimental import pallas as pl
from jax.experimental.pallas import tpu as pltpu
from jax.sharding import PartitionSpec as P

BLOCK = 128


def pair_lists(block_count):
    query_list = []
    key_list = []
    for query_block in range(block_count):
        for key_block in range(query_block + 1):
            query_list.append(query_block)
            key_list.append(key_block)
    return (np.array(query_list, np.int32), np.array(key_list, np.int32))


def live_pairs(seg_window, query_list, key_list, tile_rows):
    first_seg = jnp.take(seg_window, query_list * tile_rows)
    last_seg = jnp.take(seg_window, key_list * tile_rows + tile_rows - 1)
    return (first_seg == last_seg) | jnp.asarray(query_list == key_list)


def pair_grads(query_tile, dout_tile, key_tile, value_tile, lse_tile, delta_tile, allowed):
    tile_rows, groups, query_width = query_tile.shape
    head_size = key_tile.shape[2]
    heads_per_group = query_width // head_size
    query_heads = query_tile.reshape(tile_rows, groups, heads_per_group, head_size)
    dout_heads = dout_tile.reshape(tile_rows, groups, heads_per_group, head_size)
    scores = jnp.einsum(
        "agrd,bgd->grab", query_heads, key_tile, preferred_element_type=jnp.float32
    ) * head_size ** (-0.5)
    logits = scores - lse_tile.astype(jnp.float32)[:, :, :, None]
    soft_probs = jnp.where(allowed[None, None], jnp.exp(logits), 0.0)
    probs_low = soft_probs.astype(jnp.bfloat16)
    value_gradient = jnp.einsum(
        "grab,agrd->bgd", probs_low, dout_heads, preferred_element_type=jnp.float32
    )
    grad_prob = jnp.einsum(
        "agrd,bgd->grab", dout_heads, value_tile, preferred_element_type=jnp.float32
    )
    grad_score = (soft_probs * (grad_prob - delta_tile.astype(jnp.float32)[:, :, :, None])).astype(
        jnp.bfloat16
    )
    query_gradient = jnp.einsum(
        "grab,bgd->agrd", grad_score, key_tile, preferred_element_type=jnp.float32
    )
    key_gradient = jnp.einsum(
        "grab,agrd->bgd", grad_score, query_heads, preferred_element_type=jnp.float32
    )
    return (query_gradient.reshape(tile_rows, groups, query_width), key_gradient, value_gradient)


def on_device(
    query_rows,
    key_rows,
    value_rows,
    output_gradient,
    row_logsumexp,
    row_delta_sums,
    segments,
    query_key_value_weight,
):
    window, kv_dev, query_width = query_rows.shape
    head_size = key_rows.shape[2]
    tile_rows = BLOCK
    block_count = window // tile_rows
    query_list, key_list = pair_lists(block_count)
    query_table = jnp.asarray(query_list)
    key_table = jnp.asarray(key_list)
    myself = lax.axis_index("tok")
    own_seg = lax.dynamic_slice_in_dim(segments, myself * window, window)
    own_live = live_pairs(own_seg, query_list, key_list, tile_rows)
    block_ids = jnp.arange(block_count, dtype=jnp.int32)
    query_match = (query_table[:, None] == block_ids[None, :]) & own_live[:, None]
    key_match = key_table[:, None] == block_ids[None, :]
    block_local = jnp.any(query_match[:, :, None] & key_match[:, None, :], axis=0)
    token_local = jnp.repeat(jnp.repeat(block_local, tile_rows, axis=0), tile_rows, axis=1)
    offsets = jnp.arange(window, dtype=jnp.int32)
    allowed_all = (
        (own_seg[:, None] == own_seg[None, :])
        & (offsets[None, :] <= offsets[:, None])
        & token_local
    )
    local_out = pair_grads(
        query_rows,
        output_gradient,
        key_rows,
        value_rows,
        row_logsumexp,
        row_delta_sums,
        allowed_all,
    )
    acc_query = local_out[0].reshape(block_count, tile_rows, kv_dev, query_width)
    acc_key = local_out[1].reshape(block_count, tile_rows, kv_dev, head_size)
    acc_value = local_out[2].reshape(block_count, tile_rows, kv_dev, head_size)
    score_scale = head_size ** (-0.5)
    query_gradient = (acc_query * score_scale).reshape(window, kv_dev, query_width)
    key_gradient = (acc_key * score_scale).reshape(window, kv_dev, head_size)
    value_gradient = acc_value.reshape(window, kv_dev, head_size)
    stacked_gradients = (
        jnp.concatenate([query_gradient, key_gradient, value_gradient], axis=2)
        .astype(jnp.bfloat16)
        .reshape(window, -1)
    )
    weight_piece = lax.all_gather(query_key_value_weight, "tok", axis=0, tiled=True)
    flat_piece = weight_piece.reshape(weight_piece.shape[0], -1)
    partial_sum = lax.dot_general(
        stacked_gradients, flat_piece, (((1,), (1,)), ((), ())), preferred_element_type=jnp.float32
    )
    summed = lax.psum_scatter(
        partial_sum.astype(jnp.bfloat16), "head", scatter_dimension=1, tiled=True
    )
    return summed


MESH = pl.DeviceIdType.MESH
LANES = 128


def fused_kernel(
    inner,
    q_ref,
    k_ref,
    v_ref,
    do_ref,
    lse_ref,
    delta_ref,
    seg_ref,
    w_ref,
    out_ref,
    joined,
    w_all,
    part,
    got,
    fwd_out,
    fwd_in,
    bias,
    lse32,
    delta32,
    dk_acc,
    dv_acc,
    w_send,
    w_recv,
    j_send,
    j_recv,
    p_send,
    p_recv,
    f_send,
    f_recv,
):
    outer, chunks = w_all.shape[0], w_all.shape[1]
    heads = outer
    window, head_size = k_ref.shape
    groups = q_ref.shape[1] // head_size
    rows = w_ref.shape[0]
    tok, h = lax.axis_index("tok"), lax.axis_index("head")
    z, y = tok // inner, tok % inner
    yo = inner - 1 - y

    def remote(src, dst, send, recv, to_tok, to_head):
        return pltpu.make_async_remote_copy(
            src_ref=src,
            dst_ref=dst,
            send_sem=send,
            recv_sem=recv,
            device_id=(to_tok, to_head),
            device_id_type=MESH,
        )

    def peer(step):
        return lax.rem(h + step, heads)

    barrier = pltpu.get_barrier_semaphore()
    pl.semaphore_signal(barrier, inc=1, device_id=(z * inner + yo, h), device_id_type=MESH)
    for step in range(1, heads):
        pl.semaphore_signal(barrier, inc=1, device_id=(tok, peer(step)), device_id_type=MESH)

    @pl.when(z > 0)
    def _():
        pl.semaphore_signal(barrier, inc=1, device_id=(tok - inner, h), device_id_type=MESH)

    @pl.when(z < outer - 1)
    def _():
        pl.semaphore_signal(barrier, inc=1, device_id=(tok + inner, h), device_id_type=MESH)

    edges = jnp.where(z > 0, 1, 0) + jnp.where(z < outer - 1, 1, 0)
    pl.semaphore_wait(barrier, heads + edges)

    def own_w(c):
        return pl.ds(pl.multiple_of(c * LANES, LANES), LANES)

    def w_copy(side, o, c, own):
        src = w_ref.at[own_w(c)] if own else w_all.at[o, c]
        move = 1 if side == 1 else -1
        return remote(
            src, w_all.at[o, c], w_send.at[side, o, c], w_recv.at[o, c], tok + move * inner, h
        )

    def can_send(side):
        return z < outer - 1 if side == 1 else z > 0

    def each_chunk(body):
        lax.fori_loop(0, chunks, lambda c, carry: (body(c), carry)[1], 0)

    @each_chunk
    def _(c):
        for side in (0, 1):

            @pl.when(can_send(side))
            def _():
                w_copy(side, z, c, True).start()

    lse32[...] = lse_ref[0].astype(jnp.float32)
    delta32[...] = delta_ref[0].astype(jnp.float32)
    seg_row = seg_ref[:, pl.ds(pl.multiple_of(tok * window, LANES), window)].astype(jnp.float32)
    seg_col = jnp.transpose(jnp.broadcast_to(seg_row, (LANES, window)))[:, :1]
    key_id = lax.broadcasted_iota(jnp.int32, (window, window), 0)
    query_id = lax.broadcasted_iota(jnp.int32, (window, window), 1)
    bias[...] = jnp.where((seg_col == seg_row) & (key_id <= query_id), 0.0, -1e30)
    dk_acc[...] = jnp.zeros_like(dk_acc)
    dv_acc[...] = jnp.zeros_like(dv_acc)
    scale = head_size ** (-0.5)
    half = window // 2

    def dot(a, b, da, db):
        return lax.dot_general(a, b, (((da,), (db,)), ((), ())), preferred_element_type=jnp.float32)

    @pl.loop(0, groups)
    def _(r):
        cols = pl.ds(pl.multiple_of(r * head_size, head_size), head_size)
        pieces = []
        for first in (0, half):
            keys, queries = slice(first, first + half), slice(first, window)
            q, do = q_ref[queries, cols], do_ref[queries, cols]
            kk, vv = k_ref[keys, :], v_ref[keys, :]
            logits = dot(kk, q, 1, 1) * scale - lse32[pl.ds(r, 1), queries]
            probs = jnp.exp(logits + bias[keys, queries])
            dv_acc[keys, :] += dot(probs.astype(jnp.bfloat16), do, 1, 0)
            grad_prob = dot(vv, do, 1, 1)
            ds = (probs * (grad_prob - delta32[pl.ds(r, 1), queries])).astype(jnp.bfloat16)
            dk_acc[keys, :] += dot(ds, q, 1, 0)
            pieces.append(dot(ds, kk, 0, 0))
        low = pieces[0]
        joined[y, :half, cols] = (low[:half] * scale).astype(jnp.bfloat16)
        joined[y, half:, cols] = ((low[half:] + pieces[1]) * scale).astype(jnp.bfloat16)

    wide = groups * head_size
    joined[y, :, wide : wide + head_size] = (dk_acc[...] * scale).astype(jnp.bfloat16)
    joined[y, :, wide + head_size : wide + 2 * head_size] = dv_acc[...].astype(jnp.bfloat16)

    def p_copy(o, c, yd):
        return remote(
            part.at[o, c, yd], got.at[h, c, yd], p_send.at[o, c, yd], p_recv.at[h, c, yd], tok, o
        )

    def piece(o, c, yd, own):
        w = w_ref[own_w(c), :] if own else w_all[o, c]
        part[o, c, yd] = dot(joined[yd], w, 1, 1).astype(jnp.bfloat16)

    def send_piece(o, c, yd):
        @pl.when(o != h)
        def _():
            p_copy(o, c, yd).start()

    def arrive(side, s, c):
        o = z + s if side == 0 else z - s
        w_copy(side, o, c, False).wait_recv()

        @pl.when(can_send(side))
        def _():
            w_copy(side, o, c, False).start()

        return o

    def valid(side, s):
        return z + s < outer if side == 0 else z >= s

    def f_copy(c):
        return remote(fwd_out.at[c], fwd_in.at[c], f_send.at[c], f_recv.at[c], z * inner + yo, h)

    def total(c, yd):
        acc = part[h, c, yd].astype(jnp.float32)
        for step in range(1, heads):
            g = peer(step)
            remote(
                part.at[h, c, yd], got.at[g, c, yd], p_send.at[h, c, yd], p_recv.at[g, c, yd], tok, g
            ).wait_recv()
            acc += got[g, c, yd].astype(jnp.float32)
        return acc.astype(jnp.bfloat16)

    def out_cols(c, yd):
        return pl.ds(pl.multiple_of(yd * rows + c * LANES, LANES), LANES)

    def reduce_chunk(c):
        fwd_out[c] = total(c, yo)
        f_copy(c).start()
        out_ref[:, out_cols(c, y)] = total(c, y)

    distance = jnp.abs(z - h)
    j_copy = remote(joined.at[y], joined.at[y], j_send, j_recv, z * inner + yo, h)
    j_copy.start()

    @each_chunk
    def _(c):
        piece(z, c, y, True)
        send_piece(z, c, y)

    @each_chunk
    def _(c):
        for side in (0, 1):

            @pl.when(valid(side, 1))
            def _():
                o = arrive(side, 1, c)
                piece(o, c, y, False)
                send_piece(o, c, y)

    remote(joined.at[yo], joined.at[yo], j_send, j_recv, z * inner + yo, h).wait_recv()

    @each_chunk
    def _(c):
        piece(z, c, yo, True)
        send_piece(z, c, yo)
        for side in (0, 1):

            @pl.when(valid(side, 1))
            def _():
                o = z + 1 if side == 0 else z - 1
                piece(o, c, yo, False)
                send_piece(o, c, yo)

    @pl.when(distance == 0)
    def _():
        each_chunk(reduce_chunk)

    for s in range(2, outer):

        @each_chunk
        def _(c):
            for side in (0, 1):

                @pl.when(valid(side, s))
                def _():
                    o = arrive(side, s, c)
                    piece(o, c, yo, False)
                    piece(o, c, y, False)
                    send_piece(o, c, yo)
                    send_piece(o, c, y)

            @pl.when(distance == s - 1)
            def _():
                reduce_chunk(c)

    @pl.when(distance == outer - 1)
    def _():
        each_chunk(reduce_chunk)

    @each_chunk
    def _(c):
        f_copy(c).wait_recv()
        out_ref[:, out_cols(c, yo)] = fwd_in[c]

    j_copy.wait_send()

    @each_chunk
    def _(c):
        f_copy(c).wait_send()
        for step in range(1, heads):
            for yd in range(inner):
                p_copy(peer(step), c, yd).wait_send()
        for side in (0, 1):
            for s in range(outer):

                @pl.when(can_send(side) & valid(side, s))
                def _():
                    w_copy(side, z + s if side == 0 else z - s, c, s == 0).wait_send()


def fused(inner, outer, q, k, v, do, lse, delta, segments, weight):
    window, _, query_width = q.shape
    head_size = k.shape[2]
    rows, _, width = weight.shape
    chunks = rows // LANES
    bf16, f32 = jnp.bfloat16, jnp.float32
    dma = pltpu.SemaphoreType.DMA
    vmem = pl.BlockSpec(memory_space=pltpu.VMEM)
    return pl.pallas_call(
        functools.partial(fused_kernel, inner),
        out_shape=jax.ShapeDtypeStruct((window, inner * rows), bf16),
        in_specs=[vmem] * 8,
        out_specs=vmem,
        scratch_shapes=[
            pltpu.VMEM((inner, window, width), bf16),
            pltpu.VMEM((outer, chunks, LANES, width), bf16),
            pltpu.VMEM((outer, chunks, inner, window, LANES), bf16),
            pltpu.VMEM((outer, chunks, inner, window, LANES), bf16),
            pltpu.VMEM((chunks, window, LANES), bf16),
            pltpu.VMEM((chunks, window, LANES), bf16),
            pltpu.VMEM((window, window), f32),
            pltpu.VMEM(lse.shape[1:], f32),
            pltpu.VMEM(lse.shape[1:], f32),
            pltpu.VMEM((window, head_size), f32),
            pltpu.VMEM((window, head_size), f32),
            dma((2, outer, chunks)),
            dma((outer, chunks)),
            dma,
            dma,
            dma((outer, chunks, inner)),
            dma((outer, chunks, inner)),
            dma((chunks,)),
            dma((chunks,)),
        ],
        compiler_params=pltpu.CompilerParams(
            collective_id=0, has_side_effects=True, vmem_limit_bytes=60 * 1024 * 1024
        ),
    )(
        q.reshape(window, query_width),
        k.reshape(window, head_size),
        v.reshape(window, head_size),
        do.reshape(window, query_width),
        lse,
        delta,
        segments.reshape(1, -1),
        weight.reshape(rows, width),
    )


def solution(mesh):
    placed = (
        P("tok", "head", None),
        P("tok", "head", None),
        P("tok", "head", None),
        P("tok", "head", None),
        P("head", None, "tok"),
        P("head", None, "tok"),
        P(),
        P("tok", "head", None),
    )
    tok, heads = mesh.shape["tok"], mesh.shape["head"]

    def step(*args):
        window, kv_dev, _ = args[0].shape
        rows = args[7].shape[0]
        paired = tok == 2 * heads and heads > 1 and kv_dev == 1
        if paired and rows % LANES == 0 and window % (2 * LANES) == 0 and args[1].shape[2] == LANES:
            return fused(tok // heads, heads, *args)
        return on_device(*args)

    return jax.shard_map(
        step, mesh=mesh, in_specs=placed, out_specs=P("tok", "head"), check_vma=False
    )
```

```python
import functools

import jax
import jax.numpy as jnp
import numpy as np
from jax import lax
from jax.experimental import pallas as pl
from jax.experimental.pallas import tpu as pltpu
from jax.sharding import PartitionSpec as P

BLOCK = 128


def pair_lists(block_count):
    query_list = []
    key_list = []
    for query_block in range(block_count):
        for key_block in range(query_block + 1):
            query_list.append(query_block)
            key_list.append(key_block)
    return (np.array(query_list, np.int32), np.array(key_list, np.int32))


def live_pairs(seg_window, query_list, key_list, tile_rows):
    first_seg = jnp.take(seg_window, query_list * tile_rows)
    last_seg = jnp.take(seg_window, key_list * tile_rows + tile_rows - 1)
    return (first_seg == last_seg) | jnp.asarray(query_list == key_list)


def pair_grads(query_tile, dout_tile, key_tile, value_tile, lse_tile, delta_tile, allowed):
    tile_rows, groups, query_width = query_tile.shape
    head_size = key_tile.shape[2]
    heads_per_group = query_width // head_size
    query_heads = query_tile.reshape(tile_rows, groups, heads_per_group, head_size)
    dout_heads = dout_tile.reshape(tile_rows, groups, heads_per_group, head_size)
    scores = jnp.einsum(
        "agrd,bgd->grab", query_heads, key_tile, preferred_element_type=jnp.float32
    ) * head_size ** (-0.5)
    logits = scores - lse_tile.astype(jnp.float32)[:, :, :, None]
    soft_probs = jnp.where(allowed[None, None], jnp.exp(logits), 0.0)
    probs_low = soft_probs.astype(jnp.bfloat16)
    value_gradient = jnp.einsum(
        "grab,agrd->bgd", probs_low, dout_heads, preferred_element_type=jnp.float32
    )
    grad_prob = jnp.einsum(
        "agrd,bgd->grab", dout_heads, value_tile, preferred_element_type=jnp.float32
    )
    grad_score = (soft_probs * (grad_prob - delta_tile.astype(jnp.float32)[:, :, :, None])).astype(
        jnp.bfloat16
    )
    query_gradient = jnp.einsum(
        "grab,bgd->agrd", grad_score, key_tile, preferred_element_type=jnp.float32
    )
    key_gradient = jnp.einsum(
        "grab,agrd->bgd", grad_score, query_heads, preferred_element_type=jnp.float32
    )
    return (query_gradient.reshape(tile_rows, groups, query_width), key_gradient, value_gradient)


def on_device(
    query_rows,
    key_rows,
    value_rows,
    output_gradient,
    row_logsumexp,
    row_delta_sums,
    segments,
    query_key_value_weight,
):
    window, kv_dev, query_width = query_rows.shape
    head_size = key_rows.shape[2]
    tile_rows = BLOCK
    block_count = window // tile_rows
    query_list, key_list = pair_lists(block_count)
    query_table = jnp.asarray(query_list)
    key_table = jnp.asarray(key_list)
    myself = lax.axis_index("tok")
    own_seg = lax.dynamic_slice_in_dim(segments, myself * window, window)
    own_live = live_pairs(own_seg, query_list, key_list, tile_rows)
    block_ids = jnp.arange(block_count, dtype=jnp.int32)
    query_match = (query_table[:, None] == block_ids[None, :]) & own_live[:, None]
    key_match = key_table[:, None] == block_ids[None, :]
    block_local = jnp.any(query_match[:, :, None] & key_match[:, None, :], axis=0)
    token_local = jnp.repeat(jnp.repeat(block_local, tile_rows, axis=0), tile_rows, axis=1)
    offsets = jnp.arange(window, dtype=jnp.int32)
    allowed_all = (
        (own_seg[:, None] == own_seg[None, :])
        & (offsets[None, :] <= offsets[:, None])
        & token_local
    )
    local_out = pair_grads(
        query_rows,
        output_gradient,
        key_rows,
        value_rows,
        row_logsumexp,
        row_delta_sums,
        allowed_all,
    )
    acc_query = local_out[0].reshape(block_count, tile_rows, kv_dev, query_width)
    acc_key = local_out[1].reshape(block_count, tile_rows, kv_dev, head_size)
    acc_value = local_out[2].reshape(block_count, tile_rows, kv_dev, head_size)
    score_scale = head_size ** (-0.5)
    query_gradient = (acc_query * score_scale).reshape(window, kv_dev, query_width)
    key_gradient = (acc_key * score_scale).reshape(window, kv_dev, head_size)
    value_gradient = acc_value.reshape(window, kv_dev, head_size)
    stacked_gradients = (
        jnp.concatenate([query_gradient, key_gradient, value_gradient], axis=2)
        .astype(jnp.bfloat16)
        .reshape(window, -1)
    )
    weight_piece = lax.all_gather(query_key_value_weight, "tok", axis=0, tiled=True)
    flat_piece = weight_piece.reshape(weight_piece.shape[0], -1)
    partial_sum = lax.dot_general(
        stacked_gradients, flat_piece, (((1,), (1,)), ((), ())), preferred_element_type=jnp.float32
    )
    summed = lax.psum_scatter(
        partial_sum.astype(jnp.bfloat16), "head", scatter_dimension=1, tiled=True
    )
    return summed


MESH = pl.DeviceIdType.MESH
LANES = 128


def fused_kernel(
    inner,
    q_ref,
    k_ref,
    v_ref,
    do_ref,
    lse_ref,
    delta_ref,
    seg_ref,
    w_ref,
    out_ref,
    joined,
    w_all,
    part,
    got,
    fwd_out,
    fwd_in,
    bias,
    lse32,
    delta32,
    dk_acc,
    dv_acc,
    w_send,
    w_recv,
    j_send,
    j_recv,
    p_send,
    p_recv,
    f_send,
    f_recv,
):
    outer, chunks = w_all.shape[0], w_all.shape[1]
    heads = outer
    window, head_size = k_ref.shape
    groups = q_ref.shape[1] // head_size
    rows = w_ref.shape[0]
    tok, h = lax.axis_index("tok"), lax.axis_index("head")
    z, y = tok // inner, tok % inner
    yo = inner - 1 - y

    def remote(src, dst, send, recv, to_tok, to_head):
        return pltpu.make_async_remote_copy(
            src_ref=src,
            dst_ref=dst,
            send_sem=send,
            recv_sem=recv,
            device_id=(to_tok, to_head),
            device_id_type=MESH,
        )

    def peer(step):
        return lax.rem(h + step, heads)

    barrier = pltpu.get_barrier_semaphore()
    pl.semaphore_signal(barrier, inc=1, device_id=(z * inner + yo, h), device_id_type=MESH)
    for step in range(1, heads):
        for to_y in (y, yo):
            pl.semaphore_signal(
                barrier, inc=1, device_id=(z * inner + to_y, peer(step)), device_id_type=MESH
            )

    @pl.when(z > 0)
    def _():
        pl.semaphore_signal(barrier, inc=1, device_id=(tok - inner, h), device_id_type=MESH)

    @pl.when(z < outer - 1)
    def _():
        pl.semaphore_signal(barrier, inc=1, device_id=(tok + inner, h), device_id_type=MESH)

    edges = jnp.where(z > 0, 1, 0) + jnp.where(z < outer - 1, 1, 0)
    pl.semaphore_wait(barrier, 2 * heads - 1 + edges)

    def own_w(c):
        return pl.ds(pl.multiple_of(c * LANES, LANES), LANES)

    def w_copy(side, o, c, own):
        src = w_ref.at[own_w(c)] if own else w_all.at[o, c]
        move = 1 if side == 1 else -1
        return remote(
            src, w_all.at[o, c], w_send.at[side, o, c], w_recv.at[o, c], tok + move * inner, h
        )

    def can_send(side):
        return z < outer - 1 if side == 1 else z > 0

    def each_chunk(body):
        lax.fori_loop(0, chunks, lambda c, carry: (body(c), carry)[1], 0)

    @each_chunk
    def _(c):
        for side in (0, 1):

            @pl.when(can_send(side))
            def _():
                w_copy(side, z, c, True).start()

    lse32[...] = lse_ref[0].astype(jnp.float32)
    delta32[...] = delta_ref[0].astype(jnp.float32)
    seg_row = seg_ref[:, pl.ds(pl.multiple_of(tok * window, LANES), window)].astype(jnp.float32)
    seg_col = jnp.transpose(jnp.broadcast_to(seg_row, (LANES, window)))[:, :1]
    key_id = lax.broadcasted_iota(jnp.int32, (window, window), 0)
    query_id = lax.broadcasted_iota(jnp.int32, (window, window), 1)
    bias[...] = jnp.where((seg_col == seg_row) & (key_id <= query_id), 0.0, -1e30)
    dk_acc[...] = jnp.zeros_like(dk_acc)
    dv_acc[...] = jnp.zeros_like(dv_acc)
    scale = head_size ** (-0.5)
    half = window // 2

    def dot(a, b, da, db):
        return lax.dot_general(a, b, (((da,), (db,)), ((), ())), preferred_element_type=jnp.float32)

    @pl.loop(0, groups)
    def _(r):
        cols = pl.ds(pl.multiple_of(r * head_size, head_size), head_size)
        pieces = []
        for first in (0, half):
            keys, queries = slice(first, first + half), slice(first, window)
            q, do = q_ref[queries, cols], do_ref[queries, cols]
            kk, vv = k_ref[keys, :], v_ref[keys, :]
            logits = dot(kk, q, 1, 1) * scale - lse32[pl.ds(r, 1), queries]
            probs = jnp.exp(logits + bias[keys, queries])
            dv_acc[keys, :] += dot(probs.astype(jnp.bfloat16), do, 1, 0)
            grad_prob = dot(vv, do, 1, 1)
            ds = (probs * (grad_prob - delta32[pl.ds(r, 1), queries])).astype(jnp.bfloat16)
            dk_acc[keys, :] += dot(ds, q, 1, 0)
            pieces.append(dot(ds, kk, 0, 0))
        low = pieces[0]
        joined[y, :half, cols] = (low[:half] * scale).astype(jnp.bfloat16)
        joined[y, half:, cols] = ((low[half:] + pieces[1]) * scale).astype(jnp.bfloat16)

    wide = groups * head_size
    joined[y, :, wide : wide + head_size] = (dk_acc[...] * scale).astype(jnp.bfloat16)
    joined[y, :, wide + head_size : wide + 2 * head_size] = dv_acc[...].astype(jnp.bfloat16)

    def p_copy(o, c, yd):
        return remote(
            part.at[o, c, yd], got.at[h, c, yd], p_send.at[o, c, yd], p_recv.at[h, c, yd], tok, o
        )

    def direct_copy(o, c, yd):
        return remote(
            part.at[o, c, yd],
            got.at[h, c, y],
            p_send.at[o, c, yd],
            p_recv.at[h, c, y],
            z * inner + yd,
            o,
        )

    def piece(o, c, yd, own):
        w = w_ref[own_w(c), :] if own else w_all[o, c]
        part[o, c, yd] = dot(joined[yd], w, 1, 1).astype(jnp.bfloat16)

    def send_piece(o, c, yd):
        @pl.when(o != h)
        def _():
            p_copy(o, c, yd).start()

    def arrive(side, s, c):
        o = z + s if side == 0 else z - s
        w_copy(side, o, c, False).wait_recv()

        @pl.when(can_send(side))
        def _():
            w_copy(side, o, c, False).start()

        return o

    def valid(side, s):
        return z + s < outer if side == 0 else z >= s

    def f_copy(c):
        return remote(fwd_out.at[c], fwd_in.at[c], f_send.at[c], f_recv.at[c], z * inner + yo, h)

    def total(c, yd):
        acc = part[h, c, yd].astype(jnp.float32)
        for step in range(1, heads):
            g = peer(step)
            remote(
                part.at[h, c, yd], got.at[g, c, yd], p_send.at[h, c, yd], p_recv.at[g, c, yd], tok, g
            ).wait_recv()
            acc += got[g, c, yd].astype(jnp.float32)
        return acc.astype(jnp.bfloat16)

    def out_cols(c, yd):
        return pl.ds(pl.multiple_of(yd * rows + c * LANES, LANES), LANES)

    def reduce_chunk(c):
        fwd_out[c] = total(c, yo)
        f_copy(c).start()
        out_ref[:, out_cols(c, y)] = total(c, y)

    distance = jnp.abs(z - h)
    j_copy = remote(joined.at[y], joined.at[y], j_send, j_recv, z * inner + yo, h)
    j_copy.start()

    @each_chunk
    def _(c):
        piece(z, c, y, True)
        send_piece(z, c, y)

    @each_chunk
    def _(c):
        for side in (0, 1):

            @pl.when(valid(side, 1))
            def _():
                o = arrive(side, 1, c)
                piece(o, c, y, False)
                send_piece(o, c, y)

    remote(joined.at[yo], joined.at[yo], j_send, j_recv, z * inner + yo, h).wait_recv()

    @each_chunk
    def _(c):
        piece(z, c, yo, True)
        send_piece(z, c, yo)
        for side in (0, 1):

            @pl.when(valid(side, 1))
            def _():
                o = z + 1 if side == 0 else z - 1
                piece(o, c, yo, False)
                send_piece(o, c, yo)

    @pl.when(distance == 0)
    def _():
        each_chunk(reduce_chunk)

    for s in range(2, outer):

        @each_chunk
        def _(c):
            for side in (0, 1):

                @pl.when(valid(side, s))
                def _():
                    o = arrive(side, s, c)
                    piece(o, c, yo, False)
                    piece(o, c, y, False)
                    if s < outer - 1:
                        send_piece(o, c, yo)
                        send_piece(o, c, y)
                    else:
                        direct_copy(o, c, yo).start()

                        @pl.when(o != h)
                        def _():
                            direct_copy(o, c, y).start()

            @pl.when(distance == s - 1)
            def _():
                reduce_chunk(c)

    def arrived(g, c, ys):
        remote(
            part.at[h, c, ys], got.at[g, c, ys], p_send.at[h, c, ys], p_recv.at[g, c, ys], tok, g
        ).wait_recv()
        return got[g, c, ys].astype(jnp.float32)

    @pl.when(distance == outer - 1)
    def _():
        @each_chunk
        def _(c):
            acc = part[h, c, y].astype(jnp.float32)
            for step in range(1, heads):
                acc += arrived(peer(step), c, y)
            out_ref[:, out_cols(c, y)] = acc.astype(jnp.bfloat16)
            other = arrived(h, c, yo)
            for step in range(1, heads):
                other += arrived(peer(step), c, yo)
            out_ref[:, out_cols(c, yo)] = other.astype(jnp.bfloat16)
            direct_copy(h, c, yo).wait_send()

    @pl.when(distance < outer - 1)
    def _():
        @each_chunk
        def _(c):
            f_copy(c).wait_recv()
            out_ref[:, out_cols(c, yo)] = fwd_in[c]
            f_copy(c).wait_send()

    j_copy.wait_send()

    @each_chunk
    def _(c):
        for step in range(1, heads):
            for yd in range(inner):
                p_copy(peer(step), c, yd).wait_send()
        for side in (0, 1):
            for s in range(outer):

                @pl.when(can_send(side) & valid(side, s))
                def _():
                    w_copy(side, z + s if side == 0 else z - s, c, s == 0).wait_send()


def fused(inner, outer, q, k, v, do, lse, delta, segments, weight):
    window, _, query_width = q.shape
    head_size = k.shape[2]
    rows, _, width = weight.shape
    chunks = rows // LANES
    bf16, f32 = jnp.bfloat16, jnp.float32
    dma = pltpu.SemaphoreType.DMA
    vmem = pl.BlockSpec(memory_space=pltpu.VMEM)
    return pl.pallas_call(
        functools.partial(fused_kernel, inner),
        out_shape=jax.ShapeDtypeStruct((window, inner * rows), bf16),
        in_specs=[vmem] * 8,
        out_specs=vmem,
        scratch_shapes=[
            pltpu.VMEM((inner, window, width), bf16),
            pltpu.VMEM((outer, chunks, LANES, width), bf16),
            pltpu.VMEM((outer, chunks, inner, window, LANES), bf16),
            pltpu.VMEM((outer, chunks, inner, window, LANES), bf16),
            pltpu.VMEM((chunks, window, LANES), bf16),
            pltpu.VMEM((chunks, window, LANES), bf16),
            pltpu.VMEM((window, window), f32),
            pltpu.VMEM(lse.shape[1:], f32),
            pltpu.VMEM(lse.shape[1:], f32),
            pltpu.VMEM((window, head_size), f32),
            pltpu.VMEM((window, head_size), f32),
            dma((2, outer, chunks)),
            dma((outer, chunks)),
            dma,
            dma,
            dma((outer, chunks, inner)),
            dma((outer, chunks, inner)),
            dma((chunks,)),
            dma((chunks,)),
        ],
        compiler_params=pltpu.CompilerParams(
            collective_id=0, has_side_effects=True, vmem_limit_bytes=60 * 1024 * 1024
        ),
    )(
        q.reshape(window, query_width),
        k.reshape(window, head_size),
        v.reshape(window, head_size),
        do.reshape(window, query_width),
        lse,
        delta,
        segments.reshape(1, -1),
        weight.reshape(rows, width),
    )


def solution(mesh):
    placed = (
        P("tok", "head", None),
        P("tok", "head", None),
        P("tok", "head", None),
        P("tok", "head", None),
        P("head", None, "tok"),
        P("head", None, "tok"),
        P(),
        P("tok", "head", None),
    )
    tok, heads = mesh.shape["tok"], mesh.shape["head"]

    def step(*args):
        window, kv_dev, _ = args[0].shape
        rows = args[7].shape[0]
        paired = tok == 2 * heads and heads > 2 and kv_dev == 1
        if paired and rows % LANES == 0 and window % (2 * LANES) == 0 and args[1].shape[2] == LANES:
            return fused(tok // heads, heads, *args)
        return on_device(*args)

    return jax.shard_map(
        step, mesh=mesh, in_specs=placed, out_specs=P("tok", "head"), check_vma=False
    )
```

```python
import functools

import jax
import jax.numpy as jnp
import numpy as np
from jax import lax
from jax.experimental import pallas as pl
from jax.experimental.pallas import tpu as pltpu
from jax.sharding import PartitionSpec as P

BLOCK = 128


def pair_lists(block_count):
    query_list = []
    key_list = []
    for query_block in range(block_count):
        for key_block in range(query_block + 1):
            query_list.append(query_block)
            key_list.append(key_block)
    return (np.array(query_list, np.int32), np.array(key_list, np.int32))


def live_pairs(seg_window, query_list, key_list, tile_rows):
    first_seg = jnp.take(seg_window, query_list * tile_rows)
    last_seg = jnp.take(seg_window, key_list * tile_rows + tile_rows - 1)
    return (first_seg == last_seg) | jnp.asarray(query_list == key_list)


def pair_grads(query_tile, dout_tile, key_tile, value_tile, lse_tile, delta_tile, allowed):
    tile_rows, groups, query_width = query_tile.shape
    head_size = key_tile.shape[2]
    heads_per_group = query_width // head_size
    query_heads = query_tile.reshape(tile_rows, groups, heads_per_group, head_size)
    dout_heads = dout_tile.reshape(tile_rows, groups, heads_per_group, head_size)
    scores = jnp.einsum(
        "agrd,bgd->grab", query_heads, key_tile, preferred_element_type=jnp.float32
    ) * head_size ** (-0.5)
    logits = scores - lse_tile.astype(jnp.float32)[:, :, :, None]
    soft_probs = jnp.where(allowed[None, None], jnp.exp(logits), 0.0)
    probs_low = soft_probs.astype(jnp.bfloat16)
    value_gradient = jnp.einsum(
        "grab,agrd->bgd", probs_low, dout_heads, preferred_element_type=jnp.float32
    )
    grad_prob = jnp.einsum(
        "agrd,bgd->grab", dout_heads, value_tile, preferred_element_type=jnp.float32
    )
    grad_score = (soft_probs * (grad_prob - delta_tile.astype(jnp.float32)[:, :, :, None])).astype(
        jnp.bfloat16
    )
    query_gradient = jnp.einsum(
        "grab,bgd->agrd", grad_score, key_tile, preferred_element_type=jnp.float32
    )
    key_gradient = jnp.einsum(
        "grab,agrd->bgd", grad_score, query_heads, preferred_element_type=jnp.float32
    )
    return (query_gradient.reshape(tile_rows, groups, query_width), key_gradient, value_gradient)


def on_device(
    query_rows,
    key_rows,
    value_rows,
    output_gradient,
    row_logsumexp,
    row_delta_sums,
    segments,
    query_key_value_weight,
):
    window, kv_dev, query_width = query_rows.shape
    head_size = key_rows.shape[2]
    tile_rows = BLOCK
    block_count = window // tile_rows
    query_list, key_list = pair_lists(block_count)
    query_table = jnp.asarray(query_list)
    key_table = jnp.asarray(key_list)
    myself = lax.axis_index("tok")
    own_seg = lax.dynamic_slice_in_dim(segments, myself * window, window)
    own_live = live_pairs(own_seg, query_list, key_list, tile_rows)
    block_ids = jnp.arange(block_count, dtype=jnp.int32)
    query_match = (query_table[:, None] == block_ids[None, :]) & own_live[:, None]
    key_match = key_table[:, None] == block_ids[None, :]
    block_local = jnp.any(query_match[:, :, None] & key_match[:, None, :], axis=0)
    token_local = jnp.repeat(jnp.repeat(block_local, tile_rows, axis=0), tile_rows, axis=1)
    offsets = jnp.arange(window, dtype=jnp.int32)
    allowed_all = (
        (own_seg[:, None] == own_seg[None, :])
        & (offsets[None, :] <= offsets[:, None])
        & token_local
    )
    local_out = pair_grads(
        query_rows,
        output_gradient,
        key_rows,
        value_rows,
        row_logsumexp,
        row_delta_sums,
        allowed_all,
    )
    acc_query = local_out[0].reshape(block_count, tile_rows, kv_dev, query_width)
    acc_key = local_out[1].reshape(block_count, tile_rows, kv_dev, head_size)
    acc_value = local_out[2].reshape(block_count, tile_rows, kv_dev, head_size)
    score_scale = head_size ** (-0.5)
    query_gradient = (acc_query * score_scale).reshape(window, kv_dev, query_width)
    key_gradient = (acc_key * score_scale).reshape(window, kv_dev, head_size)
    value_gradient = acc_value.reshape(window, kv_dev, head_size)
    stacked_gradients = (
        jnp.concatenate([query_gradient, key_gradient, value_gradient], axis=2)
        .astype(jnp.bfloat16)
        .reshape(window, -1)
    )
    weight_piece = lax.all_gather(query_key_value_weight, "tok", axis=0, tiled=True)
    flat_piece = weight_piece.reshape(weight_piece.shape[0], -1)
    partial_sum = lax.dot_general(
        stacked_gradients, flat_piece, (((1,), (1,)), ((), ())), preferred_element_type=jnp.float32
    )
    summed = lax.psum_scatter(
        partial_sum.astype(jnp.bfloat16), "head", scatter_dimension=1, tiled=True
    )
    return summed


MESH = pl.DeviceIdType.MESH
LANES = 128


def fused_kernel(
    inner,
    q_ref,
    k_ref,
    v_ref,
    do_ref,
    lse_ref,
    delta_ref,
    seg_ref,
    w_ref,
    out_ref,
    joined,
    w_all,
    part,
    got,
    fwd_out,
    fwd_in,
    bias,
    lse32,
    delta32,
    dk_acc,
    dv_acc,
    w_send,
    w_recv,
    j_send,
    j_recv,
    p_send,
    p_recv,
    f_send,
    f_recv,
):
    outer, chunks = w_all.shape[0], w_all.shape[1]
    heads = outer
    window, head_size = k_ref.shape
    groups = q_ref.shape[1] // head_size
    rows = w_ref.shape[0]
    tok, h = lax.axis_index("tok"), lax.axis_index("head")
    z, y = tok // inner, tok % inner
    yo = inner - 1 - y

    def remote(src, dst, send, recv, to_tok, to_head):
        return pltpu.make_async_remote_copy(
            src_ref=src,
            dst_ref=dst,
            send_sem=send,
            recv_sem=recv,
            device_id=(to_tok, to_head),
            device_id_type=MESH,
        )

    def peer(step):
        return lax.rem(h + step, heads)

    barrier = pltpu.get_barrier_semaphore()
    pl.semaphore_signal(barrier, inc=1, device_id=(z * inner + yo, h), device_id_type=MESH)
    for step in range(1, heads):
        for to_y in (y, yo):
            pl.semaphore_signal(
                barrier, inc=1, device_id=(z * inner + to_y, peer(step)), device_id_type=MESH
            )

    @pl.when(z > 0)
    def _():
        pl.semaphore_signal(barrier, inc=1, device_id=(tok - inner, h), device_id_type=MESH)

    @pl.when(z < outer - 1)
    def _():
        pl.semaphore_signal(barrier, inc=1, device_id=(tok + inner, h), device_id_type=MESH)

    edges = jnp.where(z > 0, 1, 0) + jnp.where(z < outer - 1, 1, 0)
    pl.semaphore_wait(barrier, 2 * heads - 1 + edges)

    def own_w(c):
        return pl.ds(pl.multiple_of(c * LANES, LANES), LANES)

    def w_copy(side, o, c, own):
        src = w_ref.at[own_w(c)] if own else w_all.at[o, c]
        move = 1 if side == 1 else -1
        return remote(
            src, w_all.at[o, c], w_send.at[side, o, c], w_recv.at[o, c], tok + move * inner, h
        )

    def can_send(side):
        return z < outer - 1 if side == 1 else z > 0

    def each_chunk(body):
        lax.fori_loop(0, chunks, lambda c, carry: (body(c), carry)[1], 0)

    @each_chunk
    def _(c):
        for side in (0, 1):

            @pl.when(can_send(side))
            def _():
                w_copy(side, z, c, True).start()

    lse32[...] = lse_ref[0].astype(jnp.float32)
    delta32[...] = delta_ref[0].astype(jnp.float32)
    seg_row = seg_ref[:, pl.ds(pl.multiple_of(tok * window, LANES), window)].astype(jnp.float32)
    seg_col = jnp.transpose(jnp.broadcast_to(seg_row, (LANES, window)))[:, :1]
    key_id = lax.broadcasted_iota(jnp.int32, (window, window), 0)
    query_id = lax.broadcasted_iota(jnp.int32, (window, window), 1)
    bias[...] = jnp.where((seg_col == seg_row) & (key_id <= query_id), 0.0, -1e30)
    dk_acc[...] = jnp.zeros_like(dk_acc)
    dv_acc[...] = jnp.zeros_like(dv_acc)
    scale = head_size ** (-0.5)
    half = window // 2

    def dot(a, b, da, db):
        return lax.dot_general(a, b, (((da,), (db,)), ((), ())), preferred_element_type=jnp.float32)

    @pl.loop(0, groups)
    def _(r):
        cols = pl.ds(pl.multiple_of(r * head_size, head_size), head_size)
        pieces = []
        for first in (0, half):
            keys, queries = slice(first, first + half), slice(first, window)
            q, do = q_ref[queries, cols], do_ref[queries, cols]
            kk, vv = k_ref[keys, :], v_ref[keys, :]
            logits = dot(kk, q, 1, 1) * scale - lse32[pl.ds(r, 1), queries]
            probs = jnp.exp(logits + bias[keys, queries])
            dv_acc[keys, :] += dot(probs.astype(jnp.bfloat16), do, 1, 0)
            grad_prob = dot(vv, do, 1, 1)
            ds = (probs * (grad_prob - delta32[pl.ds(r, 1), queries])).astype(jnp.bfloat16)
            dk_acc[keys, :] += dot(ds, q, 1, 0)
            pieces.append(dot(ds, kk, 0, 0))
        low = pieces[0]
        joined[y, :half, cols] = (low[:half] * scale).astype(jnp.bfloat16)
        joined[y, half:, cols] = ((low[half:] + pieces[1]) * scale).astype(jnp.bfloat16)

    wide = groups * head_size
    joined[y, :, wide : wide + head_size] = (dk_acc[...] * scale).astype(jnp.bfloat16)
    joined[y, :, wide + head_size : wide + 2 * head_size] = dv_acc[...].astype(jnp.bfloat16)

    def p_copy(o, c, yd):
        return remote(
            part.at[o, c, yd], got.at[h, c, yd], p_send.at[o, c, yd], p_recv.at[h, c, yd], tok, o
        )

    def direct_copy(o, c, yd):
        return remote(
            part.at[o, c, yd],
            got.at[h, c, y],
            p_send.at[o, c, yd],
            p_recv.at[h, c, y],
            z * inner + yd,
            o,
        )

    def piece(o, c, yd, own):
        w = w_ref[own_w(c), :] if own else w_all[o, c]
        part[o, c, yd] = dot(joined[yd], w, 1, 1).astype(jnp.bfloat16)

    def send_piece(o, c, yd):
        @pl.when(o != h)
        def _():
            p_copy(o, c, yd).start()

    def arrive(side, s, c):
        o = z + s if side == 0 else z - s
        w_copy(side, o, c, False).wait_recv()

        @pl.when(can_send(side))
        def _():
            w_copy(side, o, c, False).start()

        return o

    def valid(side, s):
        return z + s < outer if side == 0 else z >= s

    def f_copy(c):
        return remote(fwd_out.at[c], fwd_in.at[c], f_send.at[c], f_recv.at[c], z * inner + yo, h)

    def total(c, yd):
        acc = part[h, c, yd].astype(jnp.float32)
        for step in range(1, heads):
            g = peer(step)
            remote(
                part.at[h, c, yd], got.at[g, c, yd], p_send.at[h, c, yd], p_recv.at[g, c, yd], tok, g
            ).wait_recv()
            acc += got[g, c, yd].astype(jnp.float32)
        return acc.astype(jnp.bfloat16)

    def out_cols(c, yd):
        return pl.ds(pl.multiple_of(yd * rows + c * LANES, LANES), LANES)

    def reduce_chunk(c):
        fwd_out[c] = total(c, yo)
        f_copy(c).start()
        out_ref[:, out_cols(c, y)] = total(c, y)

    distance = jnp.abs(z - h)
    j_copy = remote(joined.at[y], joined.at[y], j_send, j_recv, z * inner + yo, h)
    j_copy.start()

    @each_chunk
    def _(c):
        piece(z, c, y, True)
        send_piece(z, c, y)

    @each_chunk
    def _(c):
        for side in (0, 1):

            @pl.when(valid(side, 1))
            def _():
                o = arrive(side, 1, c)
                piece(o, c, y, False)
                send_piece(o, c, y)

    remote(joined.at[yo], joined.at[yo], j_send, j_recv, z * inner + yo, h).wait_recv()

    @each_chunk
    def _(c):
        piece(z, c, yo, True)
        send_piece(z, c, yo)
        for side in (0, 1):

            @pl.when(valid(side, 1))
            def _():
                o = z + 1 if side == 0 else z - 1
                piece(o, c, yo, False)
                send_piece(o, c, yo)

    @pl.when(distance == 0)
    def _():
        each_chunk(reduce_chunk)

    for s in range(2, outer):

        @each_chunk
        def _(c):
            for side in (0, 1):

                @pl.when(valid(side, s))
                def _():
                    o = arrive(side, s, c)
                    piece(o, c, yo, False)
                    piece(o, c, y, False)
                    if s < outer - 1:
                        send_piece(o, c, yo)
                        send_piece(o, c, y)
                    else:
                        direct_copy(o, c, yo).start()

                        @pl.when(o != h)
                        def _():
                            direct_copy(o, c, y).start()

            @pl.when(distance == s - 1)
            def _():
                reduce_chunk(c)

    def arrived(g, c, ys):
        remote(
            part.at[h, c, ys], got.at[g, c, ys], p_send.at[h, c, ys], p_recv.at[g, c, ys], tok, g
        ).wait_recv()
        return got[g, c, ys].astype(jnp.float32)

    @pl.when(distance == outer - 1)
    def _():
        @each_chunk
        def _(c):
            acc = part[h, c, y].astype(jnp.float32)
            for step in range(1, heads):
                acc += arrived(peer(step), c, y)
            out_ref[:, out_cols(c, y)] = acc.astype(jnp.bfloat16)
            other = arrived(h, c, yo)
            for step in range(1, heads):
                other += arrived(peer(step), c, yo)
            out_ref[:, out_cols(c, yo)] = other.astype(jnp.bfloat16)
            direct_copy(h, c, yo).wait_send()

    @pl.when(distance < outer - 1)
    def _():
        @each_chunk
        def _(c):
            f_copy(c).wait_recv()
            out_ref[:, out_cols(c, yo)] = fwd_in[c]
            f_copy(c).wait_send()

    j_copy.wait_send()

    @each_chunk
    def _(c):
        for step in range(1, heads):
            for yd in range(inner):
                p_copy(peer(step), c, yd).wait_send()
        for side in (0, 1):
            for s in range(outer):

                @pl.when(can_send(side) & valid(side, s))
                def _():
                    w_copy(side, z + s if side == 0 else z - s, c, s == 0).wait_send()


def fused(inner, outer, q, k, v, do, lse, delta, segments, weight):
    window, _, query_width = q.shape
    head_size = k.shape[2]
    rows, _, width = weight.shape
    chunks = rows // LANES
    bf16, f32 = jnp.bfloat16, jnp.float32
    dma = pltpu.SemaphoreType.DMA
    vmem = pl.BlockSpec(memory_space=pltpu.VMEM)
    return pl.pallas_call(
        functools.partial(fused_kernel, inner),
        out_shape=jax.ShapeDtypeStruct((window, inner * rows), bf16),
        in_specs=[vmem] * 8,
        out_specs=vmem,
        scratch_shapes=[
            pltpu.VMEM((inner, window, width), bf16),
            pltpu.VMEM((outer, chunks, LANES, width), bf16),
            pltpu.VMEM((outer, chunks, inner, window, LANES), bf16),
            pltpu.VMEM((outer, chunks, inner, window, LANES), bf16),
            pltpu.VMEM((chunks, window, LANES), bf16),
            pltpu.VMEM((chunks, window, LANES), bf16),
            pltpu.VMEM((window, window), f32),
            pltpu.VMEM(lse.shape[1:], f32),
            pltpu.VMEM(lse.shape[1:], f32),
            pltpu.VMEM((window, head_size), f32),
            pltpu.VMEM((window, head_size), f32),
            dma((2, outer, chunks)),
            dma((outer, chunks)),
            dma,
            dma,
            dma((outer, chunks, inner)),
            dma((outer, chunks, inner)),
            dma((chunks,)),
            dma((chunks,)),
        ],
        compiler_params=pltpu.CompilerParams(
            collective_id=0, has_side_effects=True, vmem_limit_bytes=36 * 1024 * 1024
        ),
    )(
        q.reshape(window, query_width),
        k.reshape(window, head_size),
        v.reshape(window, head_size),
        do.reshape(window, query_width),
        lse,
        delta,
        segments.reshape(1, -1),
        weight.reshape(rows, width),
    )


def solution(mesh):
    placed = (
        P("tok", "head", None),
        P("tok", "head", None),
        P("tok", "head", None),
        P("tok", "head", None),
        P("head", None, "tok"),
        P("head", None, "tok"),
        P(),
        P("tok", "head", None),
    )
    tok, heads = mesh.shape["tok"], mesh.shape["head"]

    def step(*args):
        window, kv_dev, _ = args[0].shape
        rows = args[7].shape[0]
        paired = tok == 2 * heads and heads > 2 and kv_dev == 1
        if paired and rows % LANES == 0 and window % (2 * LANES) == 0 and args[1].shape[2] == LANES:
            return fused(tok // heads, heads, *args)
        return on_device(*args)

    return jax.shard_map(
        step, mesh=mesh, in_specs=placed, out_specs=P("tok", "head"), check_vma=False
    )
```
